8 devices in a mesh: rep: 1 (over z), dp: 8 (over x, y, core).
Axes of the slice: x: 2, y: 2, z: 1, core: 2. Of those that a mesh axis runs over, the one named last changes fastest.
Arguments:
- a: bfloat16 [8, 4, 4096, 1536], P(('rep', 'dp'))
- g: bfloat16 [8, 4, 4096, 4224], P(('rep', 'dp'))
Outputs:
- output: bfloat16 [4, 1536, 4224], P('rep')
All inputs are finite; a program needn't handle non-finite values.
Results may differ from the reference program's by a relative error of at most 0.012.
Values are sent between devices in bfloat16 or wider.
A program may use at most 2 GiB of HBM per device.

```python
import jax
import jax.numpy as jnp
from jax import lax

DEVICES = 8
MATRICES = 4
TOKENS = 4096
D = 1536
FF = 4224


def setup_inputs(seed: int = 0, part: int = 0) -> dict:
    ka, kg, ks = (jax.random.fold_in(k, part) for k in jax.random.split(jax.random.key(seed), 3))
    size = 2.0 ** jax.random.uniform(ks, (DEVICES, MATRICES, 1, 1), jnp.float32, -1.0, 1.0)
    a = jax.random.normal(ka, (DEVICES, MATRICES, TOKENS, D), jnp.float32)
    g = size * jax.random.normal(kg, (DEVICES, MATRICES, TOKENS, FF), jnp.float32) * (DEVICES * TOKENS) ** -0.5
    return {"a": a.astype(jnp.bfloat16), "g": g.astype(jnp.bfloat16)}


def reference(a, g):
    def take(so_far, one):
        return so_far + jnp.einsum("ntd,ntf->ndf", *one, preferred_element_type=jnp.float32), None

    return lax.scan(take, jnp.zeros((MATRICES, D, FF), jnp.float32), (a, g))[0].astype(jnp.bfloat16)
```

```python
import jax
import jax.numpy as jnp
from jax import lax
from jax.experimental import pallas as pl
from jax.experimental.pallas import tpu as pltpu
from jax.sharding import PartitionSpec as P

MESH = pl.DeviceIdType.MESH
W = 256
G_SLOTS = 3
F32, BF16 = jnp.float32, jnp.bfloat16
LAG2, LAG3, LAG4, LAG5, LAG6 = 1, 2, 3, 5, 7


def _kernel(
    a, g, out,
    a_buf, g_buf, pair_send, own, pair_recv,
    send1, keep1, recv1, send2, keep2, recv2, fin,
    a_sem, g_sem, pair_ss, pair_rs, ss1, rs1, ss2, rs2, loc, gs1, gr1, gs2, gr2, fs, fr,
):
    mats, rows, cols = out.shape
    half, quarter = rows // 2, rows // 8
    eighth = quarter // 2
    per = pl.cdiv(cols, W)
    last_w = cols - (per - 1) * W
    chunks = mats * per

    me = lax.axis_index("dp")
    c, y, x = lax.rem(me, 2), lax.rem(me // 2, 2), me // 4
    xn = {"dp": (1 - x) * 4 + y * 2 + c}
    yn = {"dp": x * 4 + (1 - y) * 2 + c}
    pn = {"dp": x * 4 + y * 2 + (1 - c)}

    barrier = pltpu.get_barrier_semaphore()
    for d in (xn, yn, pn):
        pl.semaphore_signal(barrier, inc=1, device_id=d, device_id_type=MESH)

    base = c * half
    p_mine, p_other = quarter * x, quarter * (1 - x)
    q_mine, q_other = 2 * quarter + quarter * y, 2 * quarter + quarter * (1 - y)

    def by_width(k, fn):
        if last_w == W:
            fn(W)
            return
        j = lax.rem(k, per)
        pl.when(j < per - 1)(lambda: fn(W))
        pl.when(j == per - 1)(lambda: fn(last_w))

    def where(k, w, start, size):
        start = pl.multiple_of(start, eighth)
        col = pl.multiple_of(lax.rem(k, per) * W, W)
        return out.at[k // per, pl.ds(start, size), pl.ds(col, w)]

    def remote(src, dst, ss, rs, to):
        return pltpu.make_async_remote_copy(
            src_ref=src, dst_ref=dst, send_sem=ss, recv_sem=rs, device_id=to, device_id_type=MESH
        )

    def load_a(n, h):
        lanes = pl.ds(pl.multiple_of(h * half, half), half)
        slot = lax.rem(n, 2)
        return pltpu.make_async_copy(a.at[0, n, :, lanes], a_buf.at[slot, :, lanes], a_sem.at[slot, h])

    def load_g(k, w):
        slot = lax.rem(k, G_SLOTS)
        col = pl.multiple_of(lax.rem(k, per) * W, W)
        return pltpu.make_async_copy(
            g.at[0, k // per, :, pl.ds(col, w)], g_buf.at[slot, :, pl.ds(0, w)], g_sem.at[slot]
        )

    def pair(k, w):
        s, r = lax.rem(k, 2), lax.rem(k, 4)
        return remote(
            pair_send.at[s, :, pl.ds(0, w)], pair_recv.at[r, :, pl.ds(0, w)], pair_ss.at[s], pair_rs.at[r], pn
        )

    def scatter1(k, w):
        s = lax.rem(k, 4)
        return [
            remote(send1.at[s, i, :, pl.ds(0, w)], recv1.at[s, i, :, pl.ds(0, w)], ss1.at[s, i], rs1.at[s, i], d)
            for i, d in enumerate((xn, yn))
        ]

    def scatter2(k, w):
        s = lax.rem(k, 4)
        return [
            remote(send2.at[s, i, :, pl.ds(0, w)], recv2.at[s, i, :, pl.ds(0, w)], ss2.at[s, i], rs2.at[s, i], d)
            for i, d in enumerate((yn, xn))
        ]

    def final_rows():
        return (base + p_mine + eighth * y, base + q_mine + eighth * x)

    def keep_local(k, w):
        s = lax.rem(k, 4)
        return [
            pltpu.make_async_copy(fin.at[s, i, :, pl.ds(0, w)], where(k, w, r, eighth), loc.at[s, i])
            for i, r in enumerate(final_rows())
        ]

    def gather1(k, w):
        s, t = lax.rem(k, 4), lax.rem(k, 8)
        return [
            remote(fin.at[s, i, :, pl.ds(0, w)], where(k, w, r, eighth), gs1.at[t, i], gr1.at[t, i], d)
            for i, (r, d) in enumerate(zip(final_rows(), (yn, xn)))
        ]

    def gather2(k, w):
        t = lax.rem(k, 8)
        return [
            remote(where(k, w, r, quarter), where(k, w, r, quarter), gs2.at[t, i], gr2.at[t, i], d)
            for i, (r, d) in enumerate(((base + p_mine, xn), (base + q_mine, yn)))
        ]

    def exchange(k, w):
        t = lax.rem(k, 8)
        return remote(where(k, w, base, half), where(k, w, base, half), fs.at[t], fr.at[t], pn)

    def matmul(k, h):
        lanes = pl.ds(pl.multiple_of(h * half, half), half)
        return lax.dot_general(
            a_buf[lax.rem(k // per, 2), :, lanes],
            g_buf[lax.rem(k, G_SLOTS)],
            (((0,), (0,)), ((), ())),
            preferred_element_type=F32,
        )

    def start(copies):
        for copy in copies:
            copy.start()

    load_a(0, 1 - c).start()
    load_g(0, W).start()
    load_a(0, c).start()
    for k in range(1, G_SLOTS - 1):
        load_g(k, W).start()
    pl.semaphore_wait(barrier, 3)

    def compute(k):
        n, j = k // per, lax.rem(k, per)

        @pl.when(k + G_SLOTS - 1 < chunks)
        def _():
            by_width(k + G_SLOTS - 1, lambda w: load_g(k + G_SLOTS - 1, w).start())

        @pl.when((j == 1) & (n + 1 < mats))
        def _():
            load_a(n + 1, 1 - c).start()
            load_a(n + 1, c).start()

        pl.when(j == 0)(lambda: load_a(n, 1 - c).wait())
        by_width(k, lambda w: load_g(k, w).wait())
        pair_send[lax.rem(k, 2)] = matmul(k, 1 - c).astype(BF16)
        by_width(k, lambda w: pair(k, w).start())
        pl.when(j == 0)(lambda: load_a(n, c).wait())
        own[...] = matmul(k, c)

        by_width(k, lambda w: pair(k, w).wait_recv())
        r, s, kept = lax.rem(k, 4), lax.rem(k, 4), lax.rem(k, 2)

        def total(first):
            span = pl.ds(pl.multiple_of(first, quarter), quarter)
            return own[span, :] + pair_recv[r, span, :].astype(F32)

        send1[s, 0] = total(p_other).astype(BF16)
        send1[s, 1] = total(q_other).astype(BF16)
        by_width(k, lambda w: start(scatter1(k, w)))
        keep1[kept, 0] = total(p_mine)
        keep1[kept, 1] = total(q_mine)

    def second(k):
        def wait(w):
            pair(k, w).wait_send()
            for copy in scatter1(k, w):
                copy.wait_recv()

        by_width(k, wait)
        s, kept = lax.rem(k, 4), lax.rem(k, 2)
        for i, bit in enumerate((y, x)):
            def total(first):
                span = pl.ds(pl.multiple_of(first, eighth), eighth)
                return keep1[kept, i, span, :] + recv1[s, i, span, :].astype(F32)

            send2[s, i] = total(eighth * (1 - bit)).astype(BF16)
            keep2[kept, i] = total(eighth * bit)
        by_width(k, lambda w: start(scatter2(k, w)))

    def third(k):
        def wait(w):
            for copy in scatter1(k, w):
                copy.wait_send()
            for copy in scatter2(k, w):
                copy.wait_recv()

        by_width(k, wait)
        s, kept = lax.rem(k, 4), lax.rem(k, 2)
        for i in range(2):
            fin[s, i] = (keep2[kept, i] + recv2[s, i].astype(F32)).astype(BF16)
        by_width(k, lambda w: start(gather1(k, w) + keep_local(k, w)))

    def fourth(k):
        def go(w):
            for copy in scatter2(k, w):
                copy.wait_send()
            for copy in keep_local(k, w):
                copy.wait()
            for copy in gather1(k, w):
                copy.wait_recv()
            start(gather2(k, w))

        by_width(k, go)

    def fifth(k):
        def go(w):
            for copy in gather1(k, w):
                copy.wait_send()
            for copy in gather2(k, w):
                copy.wait_recv()
            exchange(k, w).start()

        by_width(k, go)

    def sixth(k):
        def go(w):
            for copy in gather2(k, w):
                copy.wait_send()
            exchange(k, w).wait()

        by_width(k, go)

    @pl.loop(0, chunks + LAG6)
    def _(i):
        pl.when(i < chunks)(lambda: compute(i))
        for lag, stage in ((LAG2, second), (LAG3, third), (LAG4, fourth), (LAG5, fifth), (LAG6, sixth)):
            pl.when((i >= lag) & (i < chunks + lag))(lambda lag=lag, stage=stage: stage(i - lag))


def solution(mesh):
    def body(a, g):
        mats, tokens, rows = a.shape[1:]
        cols = g.shape[-1]
        half, quarter = rows // 2, rows // 8
        eighth = quarter // 2
        dma = pltpu.SemaphoreType.DMA
        any_space = pl.BlockSpec(memory_space=pl.ANY)
        return pl.pallas_call(
            _kernel,
            out_shape=jax.ShapeDtypeStruct((mats, rows, cols), BF16),
            in_specs=[any_space, any_space],
            out_specs=any_space,
            scratch_shapes=[
                pltpu.VMEM((2, tokens, rows), BF16),
                pltpu.VMEM((G_SLOTS, tokens, W), BF16),
                pltpu.VMEM((2, half, W), BF16),
                pltpu.VMEM((half, W), F32),
                pltpu.VMEM((4, half, W), BF16),
                pltpu.VMEM((4, 2, quarter, W), BF16),
                pltpu.VMEM((2, 2, quarter, W), F32),
                pltpu.VMEM((4, 2, quarter, W), BF16),
                pltpu.VMEM((4, 2, eighth, W), BF16),
                pltpu.VMEM((2, 2, eighth, W), F32),
                pltpu.VMEM((4, 2, eighth, W), BF16),
                pltpu.VMEM((4, 2, eighth, W), BF16),
                dma((2, 2)), dma((G_SLOTS,)), dma((2,)), dma((4,)),
                dma((4, 2)), dma((4, 2)), dma((4, 2)), dma((4, 2)), dma((4, 2)),
                dma((8, 2)), dma((8, 2)), dma((8, 2)), dma((8, 2)), dma((8,)), dma((8,)),
            ],
            compiler_params=pltpu.CompilerParams(
                collective_id=0, has_side_effects=True, vmem_limit_bytes=60 * 1024 * 1024
            ),
        )(a, g)

    spec = P(("rep", "dp"), None, None, None)
    return jax.shard_map(
        body, mesh=mesh, in_specs=(spec, spec), out_specs=P("rep", None, None), check_vma=False
    )
```

```python
import jax
import jax.numpy as jnp
from jax import lax
from jax.experimental import pallas as pl
from jax.experimental.pallas import tpu as pltpu
from jax.sharding import PartitionSpec as P

MESH = pl.DeviceIdType.MESH
W = 256
G_SLOTS = 3
F32, BF16 = jnp.float32, jnp.bfloat16
LAG1, LAG2, LAG3, LAG4, LAG5, LAG6 = 0, 1, 2, 3, 5, 7
PAIRS, KEEPS, RING, SEMS = 2, 2, 4, 8


def _kernel(
    a, g, out,
    a_buf, g_buf, pair_send, product, pair_recv,
    send1, keep1, recv1, send2, keep2, recv2, fin,
    a_sem, g_sem, pair_ss, pair_rs, ss1, rs1, ss2, rs2, loc, gs1, gr1, gs2, gr2, fs, fr,
):
    mats, rows, cols = out.shape
    half, quarter = rows // 2, rows // 8
    eighth = quarter // 2
    per = pl.cdiv(cols, W)
    last_w = cols - (per - 1) * W
    chunks = mats * per

    me = lax.axis_index("dp")
    c, y, x = lax.rem(me, 2), lax.rem(me // 2, 2), me // 4
    xn = {"dp": (1 - x) * 4 + y * 2 + c}
    yn = {"dp": x * 4 + (1 - y) * 2 + c}
    pn = {"dp": x * 4 + y * 2 + (1 - c)}

    barrier = pltpu.get_barrier_semaphore()
    for d in (xn, yn, pn):
        pl.semaphore_signal(barrier, inc=1, device_id=d, device_id_type=MESH)

    base = c * half
    p_mine, p_other = quarter * x, quarter * (1 - x)
    q_mine, q_other = 2 * quarter + quarter * y, 2 * quarter + quarter * (1 - y)

    def by_width(k, fn):
        if last_w == W:
            fn(W)
            return
        j = lax.rem(k, per)
        pl.when(j < per - 1)(lambda: fn(W))
        pl.when(j == per - 1)(lambda: fn(last_w))

    def where(k, w, start, size):
        start = pl.multiple_of(start, eighth)
        col = pl.multiple_of(lax.rem(k, per) * W, W)
        return out.at[k // per, pl.ds(start, size), pl.ds(col, w)]

    def remote(src, dst, ss, rs, to):
        return pltpu.make_async_remote_copy(
            src_ref=src, dst_ref=dst, send_sem=ss, recv_sem=rs, device_id=to, device_id_type=MESH
        )

    def load_a(n, h):
        lanes = pl.ds(pl.multiple_of(h * half, half), half)
        slot = lax.rem(n, 2)
        return pltpu.make_async_copy(a.at[0, n, :, lanes], a_buf.at[slot, :, lanes], a_sem.at[slot, h])

    def load_g(k, w):
        slot = lax.rem(k, G_SLOTS)
        col = pl.multiple_of(lax.rem(k, per) * W, W)
        return pltpu.make_async_copy(
            g.at[0, k // per, :, pl.ds(col, w)], g_buf.at[slot, :, pl.ds(0, w)], g_sem.at[slot]
        )

    def pair(k, w):
        s, r = lax.rem(k, PAIRS), lax.rem(k, RING)
        return remote(
            pair_send.at[s, :, pl.ds(0, w)], pair_recv.at[r, :, pl.ds(0, w)], pair_ss.at[s], pair_rs.at[r], pn
        )

    def scatter1(k, w):
        s = lax.rem(k, RING)
        return [
            remote(send1.at[s, i, :, pl.ds(0, w)], recv1.at[s, i, :, pl.ds(0, w)], ss1.at[s, i], rs1.at[s, i], d)
            for i, d in enumerate((xn, yn))
        ]

    def scatter2(k, w):
        s = lax.rem(k, RING)
        return [
            remote(send2.at[s, i, :, pl.ds(0, w)], recv2.at[s, i, :, pl.ds(0, w)], ss2.at[s, i], rs2.at[s, i], d)
            for i, d in enumerate((yn, xn))
        ]

    def final_rows():
        return (base + p_mine + eighth * y, base + q_mine + eighth * x)

    def keep_local(k, w):
        s = lax.rem(k, RING)
        return [
            pltpu.make_async_copy(fin.at[s, i, :, pl.ds(0, w)], where(k, w, r, eighth), loc.at[s, i])
            for i, r in enumerate(final_rows())
        ]

    def gather1(k, w):
        s, t = lax.rem(k, RING), lax.rem(k, SEMS)
        return [
            remote(fin.at[s, i, :, pl.ds(0, w)], where(k, w, r, eighth), gs1.at[t, i], gr1.at[t, i], d)
            for i, (r, d) in enumerate(zip(final_rows(), (yn, xn)))
        ]

    def gather2(k, w):
        t = lax.rem(k, SEMS)
        return [
            remote(where(k, w, r, quarter), where(k, w, r, quarter), gs2.at[t, i], gr2.at[t, i], d)
            for i, (r, d) in enumerate(((base + p_mine, xn), (base + q_mine, yn)))
        ]

    def exchange(k, w):
        t = lax.rem(k, SEMS)
        return remote(where(k, w, base, half), where(k, w, base, half), fs.at[t], fr.at[t], pn)

    def matmul(k, h):
        lanes = pl.ds(pl.multiple_of(h * half, half), half)
        return lax.dot_general(
            a_buf[lax.rem(k // per, 2), :, lanes],
            g_buf[lax.rem(k, G_SLOTS)],
            (((0,), (0,)), ((), ())),
            preferred_element_type=F32,
        )

    def start(copies):
        for copy in copies:
            copy.start()

    load_a(0, 1 - c).start()
    load_g(0, W).start()
    load_a(0, c).start()
    for k in range(1, G_SLOTS - 1):
        load_g(k, W).start()
    pl.semaphore_wait(barrier, 3)

    def compute(k):
        n, j = k // per, lax.rem(k, per)

        @pl.when(k + G_SLOTS - 1 < chunks)
        def _():
            by_width(k + G_SLOTS - 1, lambda w: load_g(k + G_SLOTS - 1, w).start())

        @pl.when((j == 1) & (n + 1 < mats))
        def _():
            load_a(n + 1, 1 - c).start()
            load_a(n + 1, c).start()

        by_width(k, lambda w: load_g(k, w).wait())

        @pl.loop(0, 2)
        def _(t):
            h = lax.rem(1 - c + t, 2)
            pl.when(j == 0)(lambda: load_a(n, h).wait())
            product[t] = matmul(k, h)

            @pl.when(t == 0)
            def _():
                pair_send[lax.rem(k, PAIRS)] = product[0].astype(BF16)
                by_width(k, lambda w: pair(k, w).start())

    def first(k):
        by_width(k, lambda w: pair(k, w).wait_recv())
        r, s, kept = lax.rem(k, RING), lax.rem(k, RING), lax.rem(k, KEEPS)

        def total(at):
            span = pl.ds(pl.multiple_of(at, quarter), quarter)
            return product[1, span, :] + pair_recv[r, span, :].astype(F32)

        send1[s, 0] = total(p_other).astype(BF16)
        send1[s, 1] = total(q_other).astype(BF16)
        by_width(k, lambda w: start(scatter1(k, w)))
        keep1[kept, 0] = total(p_mine)
        keep1[kept, 1] = total(q_mine)

    def second(k):
        def wait(w):
            pair(k, w).wait_send()
            for copy in scatter1(k, w):
                copy.wait_recv()

        by_width(k, wait)
        s, kept = lax.rem(k, RING), lax.rem(k, KEEPS)
        for i, bit in enumerate((y, x)):
            def total(at):
                span = pl.ds(pl.multiple_of(at, eighth), eighth)
                return keep1[kept, i, span, :] + recv1[s, i, span, :].astype(F32)

            send2[s, i] = total(eighth * (1 - bit)).astype(BF16)
            keep2[kept, i] = total(eighth * bit)
        by_width(k, lambda w: start(scatter2(k, w)))

    def third(k):
        def wait(w):
            for copy in scatter1(k, w):
                copy.wait_send()
            for copy in scatter2(k, w):
                copy.wait_recv()

        by_width(k, wait)
        s, kept = lax.rem(k, RING), lax.rem(k, KEEPS)
        for i in range(2):
            fin[s, i] = (keep2[kept, i] + recv2[s, i].astype(F32)).astype(BF16)
        by_width(k, lambda w: start(gather1(k, w) + keep_local(k, w)))

    def fourth(k):
        def go(w):
            for copy in scatter2(k, w):
                copy.wait_send()
            for copy in keep_local(k, w):
                copy.wait()
            for copy in gather1(k, w):
                copy.wait_recv()
            start(gather2(k, w))

        by_width(k, go)

    def fifth(k):
        def go(w):
            for copy in gather1(k, w):
                copy.wait_send()
            for copy in gather2(k, w):
                copy.wait_recv()
            exchange(k, w).start()

        by_width(k, go)

    def sixth(k):
        def go(w):
            for copy in gather2(k, w):
                copy.wait_send()
            exchange(k, w).wait()

        by_width(k, go)

    @pl.loop(0, chunks + LAG6)
    def _(i):
        pl.when(i < chunks)(lambda: compute(i))
        for lag, stage in ((LAG1, first), (LAG2, second), (LAG3, third), (LAG4, fourth), (LAG5, fifth), (LAG6, sixth)):
            pl.when((i >= lag) & (i < chunks + lag))(lambda lag=lag, stage=stage: stage(i - lag))


def solution(mesh):
    def body(a, g):
        mats, tokens, rows = a.shape[1:]
        cols = g.shape[-1]
        half, quarter = rows // 2, rows // 8
        eighth = quarter // 2
        dma = pltpu.SemaphoreType.DMA
        any_space = pl.BlockSpec(memory_space=pl.ANY)
        return pl.pallas_call(
            _kernel,
            out_shape=jax.ShapeDtypeStruct((mats, rows, cols), BF16),
            in_specs=[any_space, any_space],
            out_specs=any_space,
            scratch_shapes=[
                pltpu.VMEM((2, tokens, rows), BF16),
                pltpu.VMEM((G_SLOTS, tokens, W), BF16),
                pltpu.VMEM((PAIRS, half, W), BF16),
                pltpu.VMEM((2, half, W), F32),
                pltpu.VMEM((RING, half, W), BF16),
                pltpu.VMEM((RING, 2, quarter, W), BF16),
                pltpu.VMEM((KEEPS, 2, quarter, W), F32),
                pltpu.VMEM((RING, 2, quarter, W), BF16),
                pltpu.VMEM((RING, 2, eighth, W), BF16),
                pltpu.VMEM((KEEPS, 2, eighth, W), F32),
                pltpu.VMEM((RING, 2, eighth, W), BF16),
                pltpu.VMEM((RING, 2, eighth, W), BF16),
                dma((2, 2)), dma((G_SLOTS,)), dma((PAIRS,)), dma((RING,)),
                dma((RING, 2)), dma((RING, 2)), dma((RING, 2)), dma((RING, 2)), dma((RING, 2)),
                dma((SEMS, 2)), dma((SEMS, 2)), dma((SEMS, 2)), dma((SEMS, 2)), dma((SEMS,)), dma((SEMS,)),
            ],
            compiler_params=pltpu.CompilerParams(
                collective_id=0, has_side_effects=True, vmem_limit_bytes=60 * 1024 * 1024
            ),
        )(a, g)

    spec = P(("rep", "dp"), None, None, None)
    return jax.shard_map(
        body, mesh=mesh, in_specs=(spec, spec), out_specs=P("rep", None, None), check_vma=False
    )
```

```python
import functools

import jax
import jax.numpy as jnp
from jax import lax
from jax.experimental import pallas as pl
from jax.experimental.pallas import tpu as pltpu
from jax.sharding import PartitionSpec as P


MESH = pl.DeviceIdType.MESH
W = 256
G_SLOTS = 3
F32, BF16 = jnp.float32, jnp.bfloat16
VMEM = 67_043_328
BLOCK, BLOCKS = 192, 16
SEGMENT = 3072
FLOPS_PER_US = 500_000_000
LAG1, LAG2, LAG3, LAG4, LAG5, LAG6, LAG7 = 0, 1, 2, 3, 3, 5, 7
PACE = 4
PAIRS, KEEPS, RING, SEMS = 2, 2, 4, 8


def _kernel(
    a, g, out, last_x0, last_y0, last_x1, last_y1,
    a_buf, g_buf, pair_send, product, pair_recv,
    send1, keep1, recv1, send2, keep2, recv2, fin,
    a_sem, g_sem, pair_ss, pair_rs, ss1, rs1, ss2, rs2, loc, gs1, gr1, gs2, gr2, fs, fr,
):
    mats, (_, rows, cols) = a.shape[1], out.shape
    half, quarter = rows // 2, rows // 8
    eighth = quarter // 2
    per = pl.cdiv(cols, W)
    last_w = cols - (per - 1) * W
    chunks, done = mats * per, (mats - 1) * per

    me = lax.axis_index("dp")
    c, y, x = lax.rem(me, 2), lax.rem(me // 2, 2), me // 4
    xn = {"dp": (1 - x) * 4 + y * 2 + c}
    yn = {"dp": x * 4 + (1 - y) * 2 + c}
    pn = {"dp": x * 4 + y * 2 + (1 - c)}

    barrier = pltpu.get_barrier_semaphore()
    for d in (xn, yn, pn):
        pl.semaphore_signal(barrier, inc=1, device_id=d, device_id_type=MESH)

    base = c * half
    p_mine, p_other = quarter * x, quarter * (1 - x)
    q_mine, q_other = 2 * quarter + quarter * y, 2 * quarter + quarter * (1 - y)

    def by_width(k, fn):
        if last_w == W:
            fn(W)
            return
        j = lax.rem(k, per)
        pl.when(j < per - 1)(lambda: fn(W))
        pl.when(j == per - 1)(lambda: fn(last_w))

    def where(k, w, start, size):
        start = pl.multiple_of(start, eighth)
        col = pl.multiple_of(lax.rem(k, per) * W, W)
        return out.at[k // per, pl.ds(start, size), pl.ds(col, w)]

    def remote(src, dst, ss, rs, to):
        return pltpu.make_async_remote_copy(
            src_ref=src, dst_ref=dst, send_sem=ss, recv_sem=rs, device_id=to, device_id_type=MESH
        )

    def by_case(k, fn):
        pl.when(k < done)(lambda: by_width(k, lambda w: fn(w, None)))
        pl.when((k >= done) & (k < done + SEGMENT // W))(lambda: fn(W, 0))
        pl.when(k >= done + SEGMENT // W)(lambda: by_width(k, lambda w: fn(w, 1)))

    def load_a(n, h):
        lanes = pl.ds(pl.multiple_of(h * half, half), half)
        slot = lax.rem(n, 2)
        return pltpu.make_async_copy(a.at[0, n, :, lanes], a_buf.at[slot, :, lanes], a_sem.at[slot, h])

    def load_g(k, w):
        slot = lax.rem(k, G_SLOTS)
        col = pl.multiple_of(lax.rem(k, per) * W, W)
        return pltpu.make_async_copy(
            g.at[0, k // per, :, pl.ds(col, w)], g_buf.at[slot, :, pl.ds(0, w)], g_sem.at[slot]
        )

    def pair(k, w):
        s, r = lax.rem(k, PAIRS), lax.rem(k, RING)
        return remote(
            pair_send.at[s, :, pl.ds(0, w)], pair_recv.at[r, :, pl.ds(0, w)], pair_ss.at[s], pair_rs.at[r], pn
        )

    def scatter1(k, w):
        s = lax.rem(k, RING)
        return [
            remote(send1.at[s, i, :, pl.ds(0, w)], recv1.at[s, i, :, pl.ds(0, w)], ss1.at[s, i], rs1.at[s, i], d)
            for i, d in enumerate((xn, yn))
        ]

    def scatter2(k, w):
        s = lax.rem(k, RING)
        return [
            remote(send2.at[s, i, :, pl.ds(0, w)], recv2.at[s, i, :, pl.ds(0, w)], ss2.at[s, i], rs2.at[s, i], d)
            for i, d in enumerate((yn, xn))
        ]

    def final_places(k, w, tail):
        if tail is not None:
            col = pl.multiple_of(lax.rem(k, per) * W - SEGMENT * tail, W)
            refs = ((last_x0, last_y0), (last_x1, last_y1))[tail]
            return [
                ref.at[pl.ds(pl.multiple_of(eighth * bit, eighth), eighth), pl.ds(col, w)]
                for ref, bit in zip(refs, (y, x))
            ]
        return [where(k, w, r, eighth) for r in (base + p_mine + eighth * y, base + q_mine + eighth * x)]

    def keep_local(k, w, tail):
        s = lax.rem(k, RING)
        return [
            pltpu.make_async_copy(fin.at[s, i, :, pl.ds(0, w)], place, loc.at[s, i])
            for i, place in enumerate(final_places(k, w, tail))
        ]

    def gather1(k, w, tail):
        s, t = lax.rem(k, RING), lax.rem(k, SEMS)
        return [
            remote(fin.at[s, i, :, pl.ds(0, w)], place, gs1.at[t, i], gr1.at[t, i], d)
            for i, (place, d) in enumerate(zip(final_places(k, w, tail), (yn, xn)))
        ]

    def gather2(k, w):
        t = lax.rem(k, SEMS)
        return [
            remote(where(k, w, r, quarter), where(k, w, r, quarter), gs2.at[t, i], gr2.at[t, i], d)
            for i, (r, d) in enumerate(((base + p_mine, xn), (base + q_mine, yn)))
        ]

    def exchange(k, w):
        t = lax.rem(k, SEMS)
        return remote(where(k, w, base, half), where(k, w, base, half), fs.at[t], fr.at[t], pn)

    def matmul(k, h):
        lanes = pl.ds(pl.multiple_of(h * half, half), half)
        return lax.dot_general(
            a_buf[lax.rem(k // per, 2), :, lanes],
            g_buf[lax.rem(k, G_SLOTS)],
            (((0,), (0,)), ((), ())),
            preferred_element_type=F32,
        )

    def start(copies):
        for copy in copies:
            copy.start()

    load_a(0, 1 - c).start()
    load_g(0, W).start()
    load_a(0, c).start()
    for k in range(1, G_SLOTS - 1):
        load_g(k, W).start()
    pl.semaphore_wait(barrier, 3)

    def compute(k):
        n, j = k // per, lax.rem(k, per)

        @pl.when(k + G_SLOTS - 1 < chunks)
        def _():
            by_width(k + G_SLOTS - 1, lambda w: load_g(k + G_SLOTS - 1, w).start())

        @pl.when((j == 1) & (n + 1 < mats))
        def _():
            load_a(n + 1, 1 - c).start()
            load_a(n + 1, c).start()

        by_width(k, lambda w: load_g(k, w).wait())

        @pl.loop(0, 2)
        def _(t):
            h = lax.rem(1 - c + t, 2)
            pl.when(j == 0)(lambda: load_a(n, h).wait())
            product[t] = matmul(k, h)

            @pl.when(t == 0)
            def _():
                pair_send[lax.rem(k, PAIRS)] = product[0].astype(BF16)
                by_width(k, lambda w: pair(k, w).start())

    def first(k):
        by_width(k, lambda w: pair(k, w).wait_recv())
        r, s, kept = lax.rem(k, RING), lax.rem(k, RING), lax.rem(k, KEEPS)

        def total(at):
            span = pl.ds(pl.multiple_of(at, quarter), quarter)
            return product[1, span, :] + pair_recv[r, span, :].astype(F32)

        send1[s, 0] = total(p_other).astype(BF16)
        send1[s, 1] = total(q_other).astype(BF16)
        by_width(k, lambda w: start(scatter1(k, w)))
        keep1[kept, 0] = total(p_mine)
        keep1[kept, 1] = total(q_mine)

    def second(k):
        def wait(w):
            pair(k, w).wait_send()
            for copy in scatter1(k, w):
                copy.wait_recv()

        by_width(k, wait)
        s, kept = lax.rem(k, RING), lax.rem(k, KEEPS)
        for i, bit in enumerate((y, x)):
            def total(at):
                span = pl.ds(pl.multiple_of(at, eighth), eighth)
                return keep1[kept, i, span, :] + recv1[s, i, span, :].astype(F32)

            send2[s, i] = total(eighth * (1 - bit)).astype(BF16)
            keep2[kept, i] = total(eighth * bit)
        by_width(k, lambda w: start(scatter2(k, w)))

    def third(k):
        def wait(w):
            for copy in scatter1(k, w):
                copy.wait_send()
            for copy in scatter2(k, w):
                copy.wait_recv()

        by_width(k, wait)
        s, kept = lax.rem(k, RING), lax.rem(k, KEEPS)
        for i in range(2):
            fin[s, i] = (keep2[kept, i] + recv2[s, i].astype(F32)).astype(BF16)
        by_case(k, lambda w, tail: start(gather1(k, w, tail) + keep_local(k, w, tail)))

    def fourth(k):
        def go(w, tail):
            for copy in scatter2(k, w):
                copy.wait_send()
            for copy in keep_local(k, w, tail) + gather1(k, w, tail):
                copy.wait()

        by_case(k, go)

    def fifth(k):
        by_width(k, lambda w: start(gather2(k, w)))

    def sixth(k):
        def go(w):
            for copy in gather2(k, w):
                copy.wait_recv()
            exchange(k, w).start()

        by_width(k, go)

    def seventh(k):
        def go(w):
            for copy in gather2(k, w):
                copy.wait_send()
            exchange(k, w).wait()

        by_width(k, go)

    paced = done // (PACE - 1) * PACE + done % (PACE - 1)

    @pl.loop(0, max(chunks + LAG4, paced + LAG7))
    def _(i):
        pl.when(i < chunks)(lambda: compute(i))
        for lag, stage in ((LAG1, first), (LAG2, second), (LAG3, third), (LAG4, fourth)):
            pl.when((i >= lag) & (i < chunks + lag))(lambda lag=lag, stage=stage: stage(i - lag))
        for lag, stage in ((LAG5, fifth), (LAG6, sixth), (LAG7, seventh)):
            @pl.when((i >= lag) & (i < paced + lag) & (lax.rem(i + PACE - lag, PACE) < PACE - 1))
            def _(lag=lag, stage=stage):
                u = i - lag
                stage(u // PACE * (PACE - 1) + lax.rem(u, PACE))


def _move(loads, stores, slots):
    for i in range(len(loads) + slots):
        if 0 <= i - slots:
            stores[i - slots].wait()
        if i < len(loads):
            loads[i].start()
        j = i - slots // 2
        if 0 <= j < len(loads):
            loads[j].wait()
            stores[j].start()


def _rows(kind, out, size):
    by, others, theirs, col = kind
    quarter, width = size
    me = lax.axis_index("dp")
    c, bit = lax.rem(me, 2), lax.rem(me // 2, 2) if by else me // 4
    bit = 1 - bit if others else bit
    row = 4 * quarter * (1 - c if theirs else c) + 2 * quarter * by + quarter * bit
    return out.at[out.shape[0] - 1, pl.ds(pl.multiple_of(row, quarter), quarter), pl.ds(col, width)]


def _copy(kinds, sums, *refs):
    blocks, (out, buf, in_sem, out_sem) = refs[: len(kinds)], refs[len(kinds) :]
    sources, targets, loads, stores = [], [], [], []
    for n in range(sums.shape[0]):
        for r in range(0, sums.shape[1], BLOCK):
            sources.append(sums.at[n, pl.ds(r, BLOCK)])
            targets.append(out.at[n, pl.ds(r, BLOCK)])
    for kind, block in zip(kinds, blocks):
        sources.append(block)
        targets.append(_rows(kind, out, block.shape))
    for i, (source, target) in enumerate(zip(sources, targets)):
        slot = i % BLOCKS
        part = buf.at[slot, :, pl.ds(0, source.shape[1])]
        loads.append(pltpu.make_async_copy(source, part, in_sem.at[slot]))
        stores.append(pltpu.make_async_copy(part, target, out_sem.at[slot]))
    _move(loads, stores, BLOCKS)


def _place(kinds, *refs):
    count = len(kinds)
    blocks, out, bufs, (in_sem, out_sem) = refs[:count], refs[count + 1], refs[count + 2 : -2], refs[-2:]
    loads, stores = [], []
    for i, (kind, block, buf) in enumerate(zip(kinds, blocks, bufs)):
        loads.append(pltpu.make_async_copy(block, buf, in_sem.at[i]))
        stores.append(pltpu.make_async_copy(buf, _rows(kind, out, block.shape), out_sem.at[i]))
    for load in loads:
        load.start()
    for load, store in zip(loads, stores):
        load.wait()
        store.start()
    for store in stores:
        store.wait()


def solution(mesh):
    any_space = pl.BlockSpec(memory_space=pl.ANY)
    dma = pltpu.SemaphoreType.DMA
    devices = mesh.shape["dp"]

    def swap(t, bit):
        return lax.ppermute(t, "dp", [(i, i ^ bit) for i in range(devices)])

    def place(out, named):
        kinds, blocks = zip(*named)
        return pl.pallas_call(
            functools.partial(_place, kinds),
            out_shape=jax.ShapeDtypeStruct(out.shape, out.dtype),
            in_specs=[any_space] * (len(blocks) + 1),
            out_specs=any_space,
            scratch_shapes=[pltpu.VMEM(t.shape, t.dtype) for t in blocks] + [dma((len(blocks),))] * 2,
            input_output_aliases={len(blocks): 0},
            compiler_params=pltpu.CompilerParams(vmem_limit_bytes=VMEM),
            cost_estimate=pl.CostEstimate(
                flops=FLOPS_PER_US * 3, bytes_accessed=4 * sum(t.size for t in blocks), transcendentals=0
            ),
        )(*blocks, out)

    def body(a, g):
        mats, tokens, rows = a.shape[1:]
        cols = g.shape[-1]
        half, quarter = rows // 2, rows // 8
        eighth = quarter // 2
        lasts = [
            jax.ShapeDtypeStruct((quarter, width), BF16)
            for width in (SEGMENT, SEGMENT, cols - SEGMENT, cols - SEGMENT)
        ]
        sums, *lasts = pl.pallas_call(
            _kernel,
            out_shape=[jax.ShapeDtypeStruct((mats - 1, rows, cols), BF16)] + lasts,
            in_specs=[any_space, any_space],
            out_specs=[any_space] * 5,
            scratch_shapes=[
                pltpu.VMEM((2, tokens, rows), BF16),
                pltpu.VMEM((G_SLOTS, tokens, W), BF16),
                pltpu.VMEM((PAIRS, half, W), BF16),
                pltpu.VMEM((2, half, W), F32),
                pltpu.VMEM((RING, half, W), BF16),
                pltpu.VMEM((RING, 2, quarter, W), BF16),
                pltpu.VMEM((KEEPS, 2, quarter, W), F32),
                pltpu.VMEM((RING, 2, quarter, W), BF16),
                pltpu.VMEM((RING, 2, eighth, W), BF16),
                pltpu.VMEM((KEEPS, 2, eighth, W), F32),
                pltpu.VMEM((RING, 2, eighth, W), BF16),
                pltpu.VMEM((RING, 2, eighth, W), BF16),
                dma((2, 2)), dma((G_SLOTS,)), dma((PAIRS,)), dma((RING,)),
                dma((RING, 2)), dma((RING, 2)), dma((RING, 2)), dma((RING, 2)), dma((RING, 2)),
                dma((SEMS, 2)), dma((SEMS, 2)), dma((SEMS, 2)), dma((SEMS, 2)), dma((SEMS,)), dma((SEMS,)),
            ],
            compiler_params=pltpu.CompilerParams(
                collective_id=0, has_side_effects=True, vmem_limit_bytes=60 * 1024 * 1024
            ),
        )(a, g)

        def kinds(part, others, theirs):
            return [(by, others, theirs, SEGMENT * part) for by in range(2)]

        mine = (lasts[:2], lasts[2:])
        others = []
        for part in range(2):
            others.append([swap(t, bit) for t, bit in zip(mine[part], (4, 2))])
        theirs = [[swap(t, 1) for t in mine[part]] for part in range(2)]
        here = [n for p in range(2) for n in kinds(p, 0, 0)]
        out = pl.pallas_call(
            functools.partial(_copy, here),
            out_shape=jax.ShapeDtypeStruct((mats, rows, cols), BF16),
            in_specs=[any_space] * (1 + len(here)),
            out_specs=any_space,
            scratch_shapes=[pltpu.VMEM((BLOCKS, BLOCK, cols), BF16), dma((BLOCKS,)), dma((BLOCKS,))],
            compiler_params=pltpu.CompilerParams(vmem_limit_bytes=VMEM),
            cost_estimate=pl.CostEstimate(
                flops=FLOPS_PER_US * 28, bytes_accessed=4 * (mats - 1) * rows * cols, transcendentals=0
            ),
        )(sums, *mine[0], *mine[1])
        theirs0 = [swap(t, 1) for t in others[0]]
        named = [n for p in range(2) for n in zip(kinds(p, 0, 1), theirs[p])]
        out = place(out, named + list(zip(kinds(0, 1, 0), others[0])))
        theirs1 = [swap(t, 1) for t in others[1]]
        out = place(out, list(zip(kinds(0, 1, 1), theirs0)) + list(zip(kinds(1, 1, 0), others[1])))
        return place(out, list(zip(kinds(1, 1, 1), theirs1)))

    spec = P(("rep", "dp"), None, None, None)
    return jax.shard_map(
        body, mesh=mesh, in_specs=(spec, spec), out_specs=P("rep", None, None), check_vma=False
    )
```
